32 devices in a mesh: gx: 4 (over y, core), gy: 4 (over z), gz: 2 (over x).
Axes of the slice: x: 2, y: 2, z: 4, core: 2. Of those that a mesh axis runs over, the one named last changes fastest.
Arguments:
- face_blocks: float32 [4, 4, 2, 6, 16384], P('gx', 'gy', 'gz'), may hold values from -6 to 6
- owner_rank: int32 [4, 4, 2, 6, 1], P('gx', 'gy', 'gz'), may hold values from 0 to 3; in each aligned block of 6 rows (0 to 5, 6 to 11, ..., all dimensions but the last counted through in order) at most 2 rows name the same one
- owner_tile: int32 [4, 4, 2, 6], P('gx', 'gy', 'gz'), may hold values from 0 to 31
- live_count: int32 [4, 4, 2], P('gx', 'gy', 'gz'), may hold values from 1 to 6, as said below
- right_side: float32 [64, 256, 256], P('gx', 'gy', 'gz'), may hold values from -8 to 8
- diagonal: float32 [64, 256, 256], P('gx', 'gy', 'gz'), may hold values from 0.05 to 1
Outputs:
- solution_field: float32 [64, 256, 256], P('gx', 'gy', 'gz')
- residual: float32 [64, 256, 256], P('gx', 'gy', 'gz')
The draws below stay inside these ranges and needn't reach their ends.
Inputs may be any that keep to these rules, and one draw needn't show every extreme that they name: `owner_rank`: on one device no owner is named by more than 2 of the 6 slots, live or not; some owner is named exactly 2 times on some devices. `live_count`: some device has all 6 slots live in every draw.
All inputs are finite; a program needn't handle non-finite values.
Results may differ from the reference program's by a relative error of at most 0.00012.
Values sent between devices are 32-bit elements; how exact they have to be, the bound alone decides.
A program may use at most 64 MiB of HBM per device.

```python
import math
import jax
import jax.numpy as jnp
import numpy as np

BLK = 128
CAP = 2
ITERS = 2
CX = 16
NB = 6
NX = 64
NY = 256
NZ = 256
N_GX = 4
N_GY = 4
N_GZ = 2


def draw_live_count(key, part):
    counts = jax.random.randint(key, (N_GX, N_GY, N_GZ), 1, NB + 1)
    return counts.at[0, 0, 0].set(NB).astype(jnp.int32)


def set_ends(array, key, smallest, largest):
    place = [jax.random.randint(jax.random.fold_in(key, axis), (), 0, length) for axis, length in enumerate(array.shape)]
    main_axis = array.shape.index(max(array.shape))
    neighbour = place[:main_axis] + [(place[main_axis] + 1) % array.shape[main_axis]] + place[main_axis + 1:]
    return array.at[tuple(place)].set(smallest).at[tuple(neighbour)].set(largest)


def block_scale(rng, dims, split, low, top_value):
    gain = 1.0
    for axis_at, parts in split:
        heights = jax.random.uniform(jax.random.fold_in(jax.random.fold_in(rng, 6), axis_at), (parts,), jnp.float32, low / len(split), top_value / len(split))
        gain = gain * jnp.repeat(jnp.exp(heights), dims[axis_at] // parts).reshape((-1,) + (1,) * (len(dims) - 1 - axis_at))
    return gain


def deal_out(key, own, number, rows, count, top, bound, skew):
    sequence = jax.random.permutation(key, count)
    packed, ordinary = portions_of(count, rows * top, bound, skew, True), portions_of(count, rows * top, bound, skew, False)
    places = jnp.arange(count)

    def named(lengths, turn):
        used = int((lengths > 0).sum())
        fixed = max(1, used // 4)
        shifted = fixed + (places - fixed + turn * (used - fixed)) % max(1, count - fixed)
        return jnp.zeros((count,), jnp.int32).at[sequence[jnp.where(places < fixed, places, shifted)]].set(jnp.asarray(lengths, jnp.int32))

    lengths = jnp.where(number % 4 == 0, named(packed, number // 4), named(ordinary, number - number // 4 - 1))
    mixed = jax.random.permutation(jax.random.fold_in(own, 3), count)
    donor, sink = mixed[0:count // 2 * 2:2], mixed[1:count // 2 * 2:2]
    margin = jnp.minimum(lengths[donor] - 1, bound - lengths[sink]) // 2
    margin = jnp.where((donor == sequence[0]) | (sink == sequence[0]) | (lengths[sink] == 0), 0, jnp.maximum(margin, 0))
    shifted = jax.random.randint(jax.random.fold_in(own, 4), (count // 2,), 0, 1 << 20) % (margin + 1)
    lengths = lengths.at[donor].add(-shifted).at[sink].add(shifted)
    members = jnp.searchsorted(jnp.cumsum(lengths), jnp.arange(rows * top), side="right").astype(jnp.int32)
    listing = members.reshape(top, rows).T
    listing = listing[jax.random.permutation(jax.random.fold_in(own, 1), rows)]
    turn = jax.random.randint(jax.random.fold_in(own, 2), (rows, 1), 0, top)
    return jnp.take_along_axis(listing, (jnp.arange(top)[None, :] + turn) % top, axis=1)


def portions_of(number_of, total, limit, slope, full):
    portions = [(1 << 20) // math.isqrt(standing ** slope) + 1 for standing in range(1, number_of + 1)]
    largest = limit if full else min(limit, max(-(-total // number_of), total * portions[0] // sum(portions)))
    least = 1 if total - largest >= number_of - 1 else 0
    given, spare = [largest] + [least] * (number_of - 1), total - largest - least * (number_of - 1)
    while spare > 0:
        movable = [i for i in range(1, number_of) if given[i] < largest] or [i for i in range(1, number_of) if given[i] < limit]
        mass, left = sum([portions[i] for i in movable]), spare
        for i in movable:
            more = min(limit - given[i], max(1, left * portions[i] // mass), spare)
            given[i] = given[i] + more
            spare = spare - more
    return np.array(given)


def scatter_about(own_key, dims, deviation, reach, split=(), held_as=jnp.bfloat16):
    values = jax.random.normal(own_key, dims, jnp.float32) * deviation
    if len(split) > 0:
        values = block_scale(own_key, dims, split, -0.22, 0.18) * values
    return jnp.clip(values, min=-reach, max=reach).astype(held_as)


def setup_inputs(seed: int = 0) -> dict:
    keys = jax.random.split(jax.random.key(seed), 7)
    face_blocks = scatter_about(keys[0], (N_GX, N_GY, N_GZ, NB, BLK * BLK), 1.0, 6.0, ((0, 4), (1, 4), (2, 2)), jnp.float32)
    owner_rank_keys = jax.random.split(jax.random.fold_in(keys[1], 1), N_GX * N_GY * N_GZ * NB // NB)
    owner_rank_turns = jax.random.permutation(jax.random.fold_in(keys[1], 3), N_GX * N_GY * N_GZ * NB // NB)
    owner_rank = jax.vmap(lambda own, number: deal_out(jax.random.fold_in(keys[1], 2), own, number, NB, N_GX, 1, CAP, 2))(owner_rank_keys, owner_rank_turns).reshape((N_GX, N_GY, N_GZ, NB, 1))
    owner_tile = set_ends(jax.random.randint(keys[2], (N_GX, N_GY, N_GZ, NB), 0, 2 * CX), jax.random.fold_in(keys[2], 1), 0, (2 * CX) - 1).astype(jnp.int32)
    live_count = draw_live_count(jax.random.fold_in(keys[6], 71), 0)
    right_side = scatter_about(keys[4], (NX, NY, NZ), 1.0, 8.0, ((0, 4), (1, 4), (2, 2)), jnp.float32)
    diagonal = jnp.clip(jnp.exp(math.log(1.0) - 2.9957323 * jax.random.uniform(keys[5], (NX, NY, NZ), jnp.float32) ** block_scale(keys[5], (NX, NY, NZ), ((0, 4), (1, 4), (2, 2)), -0.2, 0.2)), 0.05, 1.0)
    return dict(face_blocks=face_blocks, owner_rank=owner_rank, owner_tile=owner_tile, live_count=live_count, right_side=right_side, diagonal=diagonal)


def restrict(values):
    half = BLK // 2
    shaped = values.reshape(values.shape[:-1] + (half, 2, half, 2))
    summed = 0.25 * jnp.sum(shaped, axis=(-3, -1))
    return summed.reshape(values.shape[:-1] + (half * half,))


def operate(field, diagonal):
    padded = jnp.pad(field, 1)
    beside = padded[2:, 1:-1, 1:-1] + padded[:-2, 1:-1, 1:-1]
    beside = beside + padded[1:-1, 2:, 1:-1] + padded[1:-1, :-2, 1:-1]
    beside = beside + padded[1:-1, 1:-1, 2:] + padded[1:-1, 1:-1, :-2]
    return (6.0 + diagonal) * field - beside


def reference(face_blocks, owner_rank, owner_tile, live_count, right_side, diagonal):
    half = BLK // 2
    restricted = restrict(face_blocks)
    slots = jnp.arange(NB, dtype=jnp.int32)
    living = (slots[None, None, None, :] < live_count[..., None]).astype(jnp.float32)
    restricted = restricted * living[..., None]
    row_y = jnp.broadcast_to(jnp.arange(N_GY, dtype=jnp.int32)[None, :, None, None], (N_GX, N_GY, N_GZ, NB))
    row_z = jnp.broadcast_to(jnp.arange(N_GZ, dtype=jnp.int32)[None, None, :, None], (N_GX, N_GY, N_GZ, NB))
    target = owner_rank[..., 0].astype(jnp.int32)
    gathered = jnp.zeros((N_GX, N_GY, N_GZ, 2 * CX, half * half), jnp.float32)
    gathered = gathered.at[target, row_y, row_z, owner_tile.astype(jnp.int32)].add(restricted)
    shaped = gathered.reshape(N_GX, N_GY, N_GZ, CX, 2, half, half)
    source = jnp.transpose(shaped, (0, 3, 1, 5, 2, 4, 6)).reshape(NX, NY, NZ)
    load = right_side + source
    solution_field = jnp.zeros_like(load)
    residual, direction = load, load
    norm_now = jnp.sum(residual * residual)
    for iteration in range(ITERS):
        image = operate(direction, diagonal)
        alpha = norm_now / jnp.sum(direction * image)
        solution_field = solution_field + alpha * direction
        residual = residual - alpha * image
        norm_next = jnp.sum(residual * residual)
        direction = residual + (norm_next / norm_now) * direction
        norm_now = norm_next
    return solution_field, residual
```

```python
import functools
import math

import jax
import jax.numpy as jnp
from jax import lax
from jax.experimental import pallas as pl
from jax.experimental.pallas import tpu as pltpu
from jax.sharding import PartitionSpec as P

CAP = 2
AXES = ("gx", "gy", "gz")
MESH = pl.DeviceIdType.MESH
F32 = jnp.float32


def offsets_of(sizes, axes):
    found = [()]
    for axis in axes:
        found = [done + (step,) for done in found for step in range(sizes[axis])]
    return [dict(zip(axes, steps)) for steps in found if any(steps)]


def stages_of(sizes):
    stages = []
    for axis in ("gx", "gz", "gy"):
        if sizes[axis] == 1:
            continue
        if stages and math.prod(sizes[a] for a in stages[-1] + [axis]) <= 8:
            stages[-1].append(axis)
        else:
            stages.append([axis])
    return stages


def kernel(
    sizes, stages,
    rank_ref, tile_ref, live_ref, face_hbm, right_hbm, diag_hbm,
    x_ref, r_ref,
    face_v, load_v, diag_v, p_v, q_v, sums_v, send_v, recv_v,
    hx_v, ysend_v, hy_v, zsend_v, hz_v, part_v, gath_v,
    in_sem, a2a_send, a2a_recv, halo_send, halo_recv, red_send, red_recv,
):
    cx, cy, cz = load_v.shape
    blocks = face_v.shape[0]
    group = sizes["gx"]
    at = {axis: lax.axis_index(axis) for axis in AXES}

    def beside(offset):
        return {a: lax.rem(at[a] + s, sizes[a]) for a, s in offset.items() if s}

    loads = [
        pltpu.make_async_copy(face_hbm, face_v, in_sem.at[0]),
        pltpu.make_async_copy(right_hbm, load_v, in_sem.at[1]),
        pltpu.make_async_copy(diag_hbm, diag_v, in_sem.at[2]),
    ]
    for copy in loads:
        copy.start()

    for number, (axis, halo) in enumerate((("gx", hx_v), ("gy", hy_v), ("gz", hz_v))):
        for side in range(2):
            @pl.when(at[axis] == (0 if side == 0 else sizes[axis] - 1))
            def _():
                for turn in range(2):
                    halo[turn, side] = jnp.zeros(halo.shape[2:], F32)

    peers = {}
    for group_axes in [["gx"], ["gy"], ["gz"]] + stages:
        for offset in offsets_of(sizes, group_axes):
            peers[tuple(offset.get(a, 0) for a in AXES)] = offset
    barrier = pltpu.get_barrier_semaphore()
    for offset in peers.values():
        pl.semaphore_signal(barrier, inc=1, device_id=beside(offset), device_id_type=MESH)

    lane = lax.broadcasted_iota(jnp.int32, (cy, cz), 1)
    lane8 = lax.broadcasted_iota(jnp.int32, (8, cz), 1)
    row = lax.broadcasted_iota(jnp.int32, (cy, cz), 0)
    right_half = lane >= cz // 2

    loads[0].wait()
    pair = (
        lax.broadcasted_iota(jnp.int32, (cz, cz), 0) // 2
        == lax.broadcasted_iota(jnp.int32, (cz, cz), 1) % (cz // 2)
    )
    pair = jnp.where(pair, 0.25, 0.0).astype(jnp.bfloat16)
    height = sums_v.shape[0] // cy
    for i in range(cy):
        sums_v[i * height:i * height + blocks, :] = (
            face_v[:, 2 * i * cz:(2 * i + 1) * cz] + face_v[:, (2 * i + 1) * cz:(2 * i + 2) * cz]
        )
        if blocks < height:
            sums_v[i * height + blocks:(i + 1) * height, :] = jnp.zeros((height - blocks, cz), F32)
    whole = sums_v[...]
    high = whole.astype(jnp.bfloat16)
    rest = whole - high.astype(F32)
    middle = rest.astype(jnp.bfloat16)
    low = (rest - middle.astype(F32)).astype(jnp.bfloat16)
    sums_v[...] = (
        jnp.dot(low, pair, preferred_element_type=F32)
        + jnp.dot(middle, pair, preferred_element_type=F32)
    ) + jnp.dot(high, pair, preferred_element_type=F32)

    target = [rank_ref[b] for b in range(blocks)]
    alive = [live_ref[0] > b for b in range(blocks)]
    position = []
    for b in range(blocks):
        count = jnp.int32(0)
        for before in range(b):
            count = count + jnp.where((target[before] == target[b]) & alive[before], 1, 0)
        position.append(count)
    for k in range(group):
        dest = lax.rem(at["gx"] + k, group)
        total = jnp.zeros((cy, cz), F32)
        tags = jnp.full((8, cz), -1.0, F32)
        for b in range(blocks):
            code = jnp.where(alive[b] & (target[b] == dest), position[b], CAP)
            left, right = jnp.where(code == 0, 1.0, 0.0), jnp.where(code == 1, 1.0, 0.0)
            weight = jnp.where(lane8 < cz // 2, left, right)
            tag = tile_ref[b].astype(F32)
            tags = jnp.where(weight > 0.5, tag, tags)
            values = sums_v[pl.ds(b, cy, stride=height), :]
            total = total + values * jnp.where(right_half, right, left)
        (recv_v if k == 0 else send_v)[k, :cy] = total
        (recv_v if k == 0 else send_v)[k, cy:] = tags

    pl.semaphore_wait(barrier, len(peers))
    exchanges = []
    for k in range(1, group):
        copy = pltpu.make_async_remote_copy(
            src_ref=send_v.at[k], dst_ref=recv_v.at[k],
            send_sem=a2a_send.at[k], recv_sem=a2a_recv.at[k],
            device_id=beside({"gx": k}), device_id_type=MESH,
        )
        copy.start()
        exchanges.append(copy)
    loads[1].wait()
    loads[2].wait()
    for copy in exchanges:
        copy.wait_recv()

    want = [(2 * x + jnp.where(lane8 >= cz // 2, 1, 0)).astype(F32)[:1] for x in range(cx)]
    order = [0, cx - 1] + list(range(1, cx - 1))

    def halo_copy(turn, axis, side, src):
        number, halo = AXES.index(axis), (hx_v, hy_v, hz_v)[AXES.index(axis)]
        step = sizes[axis] - 1 if side == 0 else 1
        return pltpu.make_async_remote_copy(
            src_ref=src, dst_ref=halo.at[turn, 1 - side],
            send_sem=halo_send.at[turn, 2 * number + side],
            recv_sem=halo_recv.at[turn, 2 * number + 1 - side],
            device_id={axis: lax.rem(at[axis] + step, sizes[axis])}, device_id_type=MESH,
        )

    def faces(turn, field, axis):
        if axis == "gx":
            return field.at[0], field.at[cx - 1]
        if axis == "gy":
            return ysend_v.at[turn, 0], ysend_v.at[turn, 1]
        return zsend_v.at[turn], zsend_v.at[turn]

    def near(axis, side):
        return at[axis] > 0 if side == 0 else at[axis] < sizes[axis] - 1

    def send(turn, field, axis):
        for side in range(2):
            @pl.when(near(axis, side))
            def _():
                halo_copy(turn, axis, side, faces(turn, field, axis)[side]).start()

    def receive(turn, field, axis):
        for side in range(2):
            @pl.when(near(axis, side))
            def _():
                halo_copy(turn, axis, 1 - side, faces(turn, field, axis)[1 - side]).wait_recv()

    def finish(turn, field, axis):
        for side in range(2):
            @pl.when(near(axis, side))
            def _():
                halo_copy(turn, axis, side, faces(turn, field, axis)[side]).wait_send()

    def pack(turn, x, plane, packed):
        ysend_v[turn, 0, x:x + 1] = plane[:1]
        ysend_v[turn, 1, x:x + 1] = plane[cy - 1:]
        turned = plane if x == 0 else pltpu.roll(plane, 2 * x, axis=1)
        return jnp.where(((lane + 1) % cz) // 2 == x, turned, packed)

    packed = jnp.zeros((cy, cz), F32)
    for x in order:
        plane = load_v[x]
        for k in range(group):
            values, tags = recv_v[k, :cy], recv_v[k, cy:cy + 1]
            plane = plane + jnp.where(tags == want[x], values, 0.0)
            plane = plane + jnp.where(
                pltpu.roll(recv_v[k, cy:], cz // 2, axis=1)[:1] == want[x],
                pltpu.roll(values, cz // 2, axis=1), 0.0,
            )
        load_v[x] = plane
        packed = pack(0, x, plane, packed)
        if x == cx - 1:
            send(0, load_v, "gx")
    zsend_v[0] = packed
    send(0, load_v, "gz")
    send(0, load_v, "gy")

    def inside(src, dst):
        for x in range(cx):
            plane = src[x]
            around = jnp.where(lane == 0, 0.0, pltpu.roll(plane, 1, axis=1))
            around = around + jnp.where(lane == cz - 1, 0.0, pltpu.roll(plane, cz - 1, axis=1))
            around = around + jnp.where(row == 0, 0.0, pltpu.roll(plane, 1, axis=0))
            around = around + jnp.where(row == cy - 1, 0.0, pltpu.roll(plane, cy - 1, axis=0))
            if x > 0:
                around = around + src[x - 1]
            if x < cx - 1:
                around = around + src[x + 1]
            dst[x] = diag_v[x] * plane - around

    def fold(acc, values):
        for part in range(cy // 8):
            acc = acc + values[8 * part:8 * part + 8]
        return acc

    def border(turn, src, dst, sink):
        for axis in ("gx", "gz", "gy"):
            receive(turn, src, axis)
        ahead, behind = hz_v[turn, 1], pltpu.roll(hz_v[turn, 0], 2, axis=1)
        merged = jnp.where(lane % 2 == 0, ahead, behind)
        for x in order:
            edge = pltpu.roll(merged, cz - 2 * x - 1, axis=1)
            plane = dst[x] - jnp.where((lane == 0) | (lane == cz - 1), edge, 0.0)
            plane = plane - jnp.where(row == 0, hy_v[turn, 0, x:x + 1], 0.0)
            plane = plane - jnp.where(row == cy - 1, hy_v[turn, 1, x:x + 1], 0.0)
            if x == 0:
                plane = plane - hx_v[turn, 0]
            if x == cx - 1:
                plane = plane - hx_v[turn, 1]
            dst[x] = plane
            sink(x, plane)

    inside(load_v, p_v)
    state = {"packed": jnp.zeros((cy, cz), F32)}

    def first(x, plane):
        state["packed"] = pack(1, x, plane, state["packed"])
        if x == cx - 1:
            send(1, p_v, "gx")

    border(0, load_v, p_v, first)
    zsend_v[1] = state["packed"]
    send(1, p_v, "gz")
    send(1, p_v, "gy")
    inside(p_v, q_v)
    acc = [jnp.zeros((8, cz), F32) for _ in range(4)]
    for x in range(cx):
        load, p = load_v[x], p_v[x]
        acc[0], acc[1], acc[2] = fold(acc[0], load * load), fold(acc[1], load * p), fold(acc[2], p * p)

    def second(x, plane):
        acc[3] = fold(acc[3], plane * p_v[x])

    border(1, p_v, q_v, second)

    row8 = lax.broadcasted_iota(jnp.int32, (8, cz), 0)
    mine = jnp.zeros((8, cz), F32)
    for number in range(4):
        mine = jnp.where(row8 == number, jnp.sum(acc[number], axis=0, keepdims=True), mine)
    slot = 0
    waiting = []
    for number, axes in enumerate(stages):
        part_v[number] = mine
        copies = []
        for offset in offsets_of(sizes, axes):
            copy = pltpu.make_async_remote_copy(
                src_ref=part_v.at[number], dst_ref=gath_v.at[slot],
                send_sem=red_send.at[slot], recv_sem=red_recv.at[slot],
                device_id=beside(offset), device_id_type=MESH,
            )
            copy.start()
            copies.append((slot, copy))
            slot += 1
        for at_slot, copy in copies:
            copy.wait_recv()
            mine = mine + gath_v[at_slot]
        waiting += [copy for _, copy in copies]

    sums = jnp.sum(mine, axis=1, keepdims=True)
    s0, s1, s2, s3 = (sums[n:n + 1] for n in range(4))
    step = 6.0 * s0 + s1
    a = s0 / step
    c = s1 / step
    norm = c * c * s0 - 2.0 * a * c * s1 + a * a * s2
    e = c + norm / s0
    curve = 6.0 * (e * e * s0 - 2.0 * e * a * s1 + a * a * s2) + (
        e * e * s1 - 2.0 * e * a * s2 + a * a * s3
    )
    b = norm / curve
    x_load, x_p = a + b * e, b * a
    r_load, r_p, r_q = c - 6.0 * b * e, a + b * (e - 6.0 * a), b * a
    for x in range(cx):
        load, p = load_v[x], p_v[x]
        x_ref[x] = x_load * load - x_p * p
        r_ref[x] = r_load * load - r_p * p + r_q * q_v[x]

    for copy in exchanges + waiting:
        copy.wait_send()
    for turn, field in ((0, load_v), (1, p_v)):
        for axis in AXES:
            finish(turn, field, axis)


def per_device(sizes, face_blocks, owner_rank, owner_tile, live_count, right_side, diagonal):
    blocks, width = face_blocks.shape[3:]
    cx, cy, cz = right_side.shape
    height = -(-blocks // 8) * 8
    group = sizes["gx"]
    stages = stages_of(sizes)
    slots = sum(len(offsets_of(sizes, axes)) for axes in stages)
    smem, vmem, anywhere = (
        pl.BlockSpec(memory_space=space) for space in (pltpu.SMEM, pltpu.VMEM, pl.ANY)
    )
    box = jax.ShapeDtypeStruct((cx, cy, cz), F32)
    return pl.pallas_call(
        functools.partial(kernel, sizes, stages),
        out_shape=(box, box),
        in_specs=[smem] * 3 + [anywhere] * 3,
        out_specs=(vmem, vmem),
        scratch_shapes=[
            pltpu.VMEM((blocks, width), F32),
            pltpu.VMEM((cx, cy, cz), F32),
            pltpu.VMEM((cx, cy, cz), F32),
            pltpu.VMEM((cx, cy, cz), F32),
            pltpu.VMEM((cx, cy, cz), F32),
            pltpu.VMEM((cy * height, cz), F32),
            pltpu.VMEM((group, cy + 8, cz), F32),
            pltpu.VMEM((group, cy + 8, cz), F32),
            pltpu.VMEM((2, 2, cy, cz), F32),
            pltpu.VMEM((2, 2, cx, cz), F32),
            pltpu.VMEM((2, 2, cx, cz), F32),
            pltpu.VMEM((2, cy, cz), F32),
            pltpu.VMEM((2, 2, cy, cz), F32),
            pltpu.VMEM((len(stages), 8, cz), F32),
            pltpu.VMEM((slots, 8, cz), F32),
            pltpu.SemaphoreType.DMA((3,)),
            pltpu.SemaphoreType.DMA((group,)),
            pltpu.SemaphoreType.DMA((group,)),
            pltpu.SemaphoreType.DMA((2, 6)),
            pltpu.SemaphoreType.DMA((2, 6)),
            pltpu.SemaphoreType.DMA((slots,)),
            pltpu.SemaphoreType.DMA((slots,)),
        ],
        compiler_params=pltpu.CompilerParams(collective_id=0, has_side_effects=True),
    )(
        owner_rank.reshape(blocks), owner_tile.reshape(blocks), live_count.reshape(1),
        face_blocks.reshape(blocks, width), right_side, diagonal,
    )


def solution(mesh):
    sizes = dict(mesh.shape)
    return jax.shard_map(
        functools.partial(per_device, sizes),
        mesh=mesh,
        in_specs=(
            P("gx", "gy", "gz", None, None),
            P("gx", "gy", "gz", None, None),
            P("gx", "gy", "gz", None),
            P("gx", "gy", "gz"),
            P("gx", "gy", "gz"),
            P("gx", "gy", "gz"),
        ),
        out_specs=(P("gx", "gy", "gz"), P("gx", "gy", "gz")),
        check_vma=False,
    )
```

```python
import functools
import math

import jax
import jax.numpy as jnp
from jax import lax
from jax.experimental import pallas as pl
from jax.experimental.pallas import tpu as pltpu
from jax.sharding import PartitionSpec as P

CAP = 2
AXES = ("gx", "gy", "gz")
MESH = pl.DeviceIdType.MESH
F32 = jnp.float32


def offsets_of(sizes, axes):
    found = [()]
    for axis in axes:
        found = [done + (step,) for done in found for step in range(sizes[axis])]
    return [dict(zip(axes, steps)) for steps in found if any(steps)]


def stages_of(sizes):
    stages = []
    for axis in ("gx", "gz", "gy"):
        if stages and math.prod(sizes[a] for a in stages[-1] + [axis]) <= 8:
            stages[-1].append(axis)
        else:
            stages.append([axis])
    return stages


def kernel(
    sizes, stages,
    rank_ref, tile_ref, live_hbm, face_hbm, right_hbm, diag_hbm,
    load_hbm, p_hbm, q_hbm, coef_ref,
    live_ref, face_v, load_v, diag_v, p_v, q_v, sums_v, send_v, recv_v, turned_v,
    hx_v, ysend_v, hy_v, zsend_v, hz_v, part_v, gath_v,
    in_sem, out_sem, a2a_send, a2a_recv, halo_send, halo_recv, red_send, red_recv,
):
    cx, cy, cz = load_v.shape
    blocks = face_v.shape[0]
    group = sizes["gx"]
    at = {axis: lax.axis_index(axis) for axis in AXES}

    def near(axis, side):
        return at[axis] > 0 if side == 0 else at[axis] < sizes[axis] - 1

    def beside(offset):
        return {a: lax.rem(at[a] + s, sizes[a]) for a, s in offset.items() if s}

    loads = [
        pltpu.make_async_copy(face_hbm, face_v, in_sem.at[0]),
        pltpu.make_async_copy(right_hbm, load_v, in_sem.at[1]),
        pltpu.make_async_copy(diag_hbm, diag_v, in_sem.at[2]),
        pltpu.make_async_copy(live_hbm, live_ref, in_sem.at[3]),
    ]
    for copy in loads:
        copy.start()

    for number, (axis, halo) in enumerate((("gx", hx_v), ("gy", hy_v), ("gz", hz_v))):
        for side in range(2):
            @pl.when(at[axis] == (0 if side == 0 else sizes[axis] - 1))
            def _():
                for turn in range(2):
                    halo[turn, side] = jnp.zeros(halo.shape[2:], F32)

    peers = {}
    for group_axes in [["gx"], ["gy"], ["gz"]] + stages:
        for offset in offsets_of(sizes, group_axes):
            peers[tuple(offset.get(a, 0) for a in AXES)] = offset
    barrier = pltpu.get_barrier_semaphore()
    for offset in peers.values():
        pl.semaphore_signal(barrier, inc=1, device_id=beside(offset), device_id_type=MESH)

    lane = lax.broadcasted_iota(jnp.int32, (cy, cz), 1)
    lane8 = lax.broadcasted_iota(jnp.int32, (8, cz), 1)
    row = lax.broadcasted_iota(jnp.int32, (cy, cz), 0)
    right_half = lane >= cz // 2

    loads[0].wait()
    loads[3].wait()
    pair = (
        lax.broadcasted_iota(jnp.int32, (cz, cz), 0) // 2
        == lax.broadcasted_iota(jnp.int32, (cz, cz), 1) % (cz // 2)
    )
    pair = jnp.where(pair, 0.25, 0.0).astype(jnp.bfloat16)
    for b in range(blocks):
        sums_v[b * cy:(b + 1) * cy] = (
            face_v[b, pl.ds(0, cy, stride=2), :] + face_v[b, pl.ds(1, cy, stride=2), :]
        )
    whole = sums_v[...]
    high = whole.astype(jnp.bfloat16)
    rest = whole - high.astype(F32)
    middle = rest.astype(jnp.bfloat16)
    low = (rest - middle.astype(F32)).astype(jnp.bfloat16)
    sums_v[...] = (
        jnp.dot(low, pair, preferred_element_type=F32)
        + jnp.dot(middle, pair, preferred_element_type=F32)
    ) + jnp.dot(high, pair, preferred_element_type=F32)

    target = [rank_ref[b] for b in range(blocks)]
    alive = [live_ref[0, 0, 0] > b for b in range(blocks)]
    position = []
    for b in range(blocks):
        count = jnp.int32(0)
        for before in range(b):
            count = count + jnp.where((target[before] == target[b]) & alive[before], 1, 0)
        position.append(count)
    for k in range(group):
        dest = lax.rem(at["gx"] + k, group)
        total = jnp.zeros((cy, cz), F32)
        tags = jnp.full((8, cz), -1.0, F32)
        for b in range(blocks):
            code = jnp.where(alive[b] & (target[b] == dest), position[b], CAP)
            left, right = jnp.where(code == 0, 1.0, 0.0), jnp.where(code == 1, 1.0, 0.0)
            weight = jnp.where(lane8 < cz // 2, left, right)
            tag = tile_ref[b].astype(F32)
            tags = jnp.where(weight > 0.5, tag, tags)
            values = sums_v[b * cy:(b + 1) * cy]
            total = total + values * jnp.where(right_half, right, left)
        (recv_v if k == 0 else send_v)[k, :cy] = total
        (recv_v if k == 0 else send_v)[k, cy:] = tags

    pl.semaphore_wait(barrier, len(peers))
    exchanges = []
    for k in range(1, group):
        copy = pltpu.make_async_remote_copy(
            src_ref=send_v.at[k], dst_ref=recv_v.at[k],
            send_sem=a2a_send.at[k], recv_sem=a2a_recv.at[k],
            device_id=beside({"gx": k}), device_id_type=MESH,
        )
        copy.start()
        exchanges.append(copy)
    loads[1].wait()
    loads[2].wait()
    for copy in exchanges:
        copy.wait_recv()

    for k in range(group):
        turned_v[k] = pltpu.roll(recv_v[k], cz // 2, axis=1)
    want = [(2 * x + jnp.where(lane8 >= cz // 2, 1, 0)).astype(F32)[:1] for x in range(cx)]
    order = [0, cx - 1] + list(range(1, cx - 1))

    def halo_copy(turn, axis, side, src):
        number, halo = AXES.index(axis), (hx_v, hy_v, hz_v)[AXES.index(axis)]
        step = sizes[axis] - 1 if side == 0 else 1
        return pltpu.make_async_remote_copy(
            src_ref=src, dst_ref=halo.at[turn, 1 - side],
            send_sem=halo_send.at[turn, 2 * number + side],
            recv_sem=halo_recv.at[turn, 2 * number + 1 - side],
            device_id={axis: lax.rem(at[axis] + step, sizes[axis])}, device_id_type=MESH,
        )

    def faces(turn, field, axis):
        if axis == "gx":
            return field.at[0], field.at[cx - 1]
        if axis == "gy":
            return ysend_v.at[turn, 0], ysend_v.at[turn, 1]
        return zsend_v.at[turn], zsend_v.at[turn]

    def send(turn, field, axis):
        for side in range(2):
            @pl.when(near(axis, side))
            def _():
                halo_copy(turn, axis, side, faces(turn, field, axis)[side]).start()

    def receive(turn, field, axis):
        for side in range(2):
            @pl.when(near(axis, side))
            def _():
                halo_copy(turn, axis, 1 - side, faces(turn, field, axis)[1 - side]).wait_recv()

    def finish(turn, field, axis):
        for side in range(2):
            @pl.when(near(axis, side))
            def _():
                halo_copy(turn, axis, side, faces(turn, field, axis)[side]).wait_send()

    def pack(turn, x, plane, packed):
        ysend_v[turn, 0, x:x + 1] = plane[:1]
        ysend_v[turn, 1, x:x + 1] = plane[cy - 1:]
        turned = plane if x == 0 else pltpu.roll(plane, 2 * x, axis=1)
        return jnp.where(((lane + 1) % cz) // 2 == x, turned, packed)

    packed = jnp.zeros((cy, cz), F32)
    for x in order:
        plane = load_v[x]
        for k in range(group):
            values, tags = recv_v[k, :cy], recv_v[k, cy:cy + 1]
            plane = plane + jnp.where(tags == want[x], values, 0.0)
            plane = plane + jnp.where(
                turned_v[k, cy:cy + 1] == want[x], turned_v[k, :cy], 0.0
            )
        load_v[x] = plane
        packed = pack(0, x, plane, packed)
        if x == cx - 1:
            send(0, load_v, "gx")
    zsend_v[0] = packed
    send(0, load_v, "gz")
    send(0, load_v, "gy")

    stores = [
        pltpu.make_async_copy(load_v, load_hbm, out_sem.at[0]),
        pltpu.make_async_copy(p_v, p_hbm, out_sem.at[1]),
        pltpu.make_async_copy(q_v, q_hbm, out_sem.at[2]),
    ]
    stores[0].start()

    def inside(src, dst):
        for x in range(cx):
            plane = src[x]
            around = jnp.where(lane == 0, 0.0, pltpu.roll(plane, 1, axis=1))
            around = around + jnp.where(lane == cz - 1, 0.0, pltpu.roll(plane, cz - 1, axis=1))
            around = around + jnp.where(row == 0, 0.0, pltpu.roll(plane, 1, axis=0))
            around = around + jnp.where(row == cy - 1, 0.0, pltpu.roll(plane, cy - 1, axis=0))
            if x > 0:
                around = around + src[x - 1]
            if x < cx - 1:
                around = around + src[x + 1]
            dst[x] = diag_v[x] * plane - around

    def fold(acc, values):
        for part in range(cy // 8):
            acc = acc + values[8 * part:8 * part + 8]
        return acc

    def border(turn, src, dst, sink):
        for axis in ("gx", "gz", "gy"):
            receive(turn, src, axis)
        ahead, behind = hz_v[turn, 1], pltpu.roll(hz_v[turn, 0], 2, axis=1)
        merged = jnp.where(lane % 2 == 0, ahead, behind)
        for x in order:
            edge = pltpu.roll(merged, cz - 2 * x - 1, axis=1)
            plane = dst[x] - jnp.where((lane == 0) | (lane == cz - 1), edge, 0.0)
            plane = plane - jnp.where(row == 0, hy_v[turn, 0, x:x + 1], 0.0)
            plane = plane - jnp.where(row == cy - 1, hy_v[turn, 1, x:x + 1], 0.0)
            if x == 0:
                plane = plane - hx_v[turn, 0]
            if x == cx - 1:
                plane = plane - hx_v[turn, 1]
            dst[x] = plane
            sink(x, plane)

    inside(load_v, p_v)
    state = {"packed": jnp.zeros((cy, cz), F32)}

    def first(x, plane):
        state["packed"] = pack(1, x, plane, state["packed"])
        if x == cx - 1:
            send(1, p_v, "gx")

    border(0, load_v, p_v, first)
    zsend_v[1] = state["packed"]
    send(1, p_v, "gz")
    send(1, p_v, "gy")
    stores[1].start()
    inside(p_v, q_v)
    acc = [jnp.zeros((8, cz), F32) for _ in range(4)]
    for x in range(cx):
        load, p = load_v[x], p_v[x]
        acc[0], acc[1], acc[2] = fold(acc[0], load * load), fold(acc[1], load * p), fold(acc[2], p * p)

    def second(x, plane):
        acc[3] = fold(acc[3], plane * p_v[x])

    border(1, p_v, q_v, second)
    stores[2].start()

    row8 = lax.broadcasted_iota(jnp.int32, (8, cz), 0)
    mine = jnp.zeros((8, cz), F32)
    for number in range(4):
        mine = jnp.where(row8 == number, jnp.sum(acc[number], axis=0, keepdims=True), mine)
    slot = 0
    waiting = []
    for number, axes in enumerate(stages):
        part_v[number] = mine
        copies = []
        for offset in offsets_of(sizes, axes):
            copy = pltpu.make_async_remote_copy(
                src_ref=part_v.at[number], dst_ref=gath_v.at[slot],
                send_sem=red_send.at[slot], recv_sem=red_recv.at[slot],
                device_id=beside(offset), device_id_type=MESH,
            )
            copy.start()
            copies.append((slot, copy))
            slot += 1
        for at_slot, copy in copies:
            copy.wait_recv()
            mine = mine + gath_v[at_slot]
        waiting += [copy for _, copy in copies]

    sums = jnp.sum(mine, axis=1, keepdims=True)
    s0, s1, s2, s3 = (sums[n:n + 1] for n in range(4))
    step = 6.0 * s0 + s1
    a = s0 / step
    c = s1 / step
    norm = c * c * s0 - 2.0 * a * c * s1 + a * a * s2
    e = c + norm / s0
    curve = 6.0 * (e * e * s0 - 2.0 * e * a * s1 + a * a * s2) + (
        e * e * s1 - 2.0 * e * a * s2 + a * a * s3
    )
    b = norm / curve
    x_load, x_p = a + b * e, b * a
    r_load, r_p, r_q = c - 6.0 * b * e, a + b * (e - 6.0 * a), b * a
    for number, value in enumerate((x_load, x_p, r_load, r_p, r_q)):
        coef_ref[number:number + 1] = jnp.broadcast_to(value, (1, cz))
    for copy in stores:
        copy.wait()
    for copy in exchanges + waiting:
        copy.wait_send()
    for turn, field in ((0, load_v), (1, p_v)):
        for axis in AXES:
            finish(turn, field, axis)


def combine(load_ref, p_ref, q_ref, coef_ref, x_ref, r_ref):
    x_load, x_p, r_load, r_p, r_q = (coef_ref[n:n + 1] for n in range(5))
    for x in range(load_ref.shape[0]):
        load, p = load_ref[x], p_ref[x]
        x_ref[x] = x_load * load - x_p * p
        r_ref[x] = r_load * load - r_p * p + r_q * q_ref[x]


def combined(load, p, q, coef):
    cx, cy, cz = load.shape
    parts = 2 if cx % 2 == 0 else 1
    piece = pl.BlockSpec((cx // parts, cy, cz), lambda i: (i, 0, 0))
    box = jax.ShapeDtypeStruct((cx, cy, cz), F32)
    return pl.pallas_call(
        combine,
        grid=(parts,),
        out_shape=(box, box),
        in_specs=[piece] * 3 + [pl.BlockSpec((8, cz), lambda i: (0, 0))],
        out_specs=(piece, piece),
    )(load, p, q, coef)


def per_device(sizes, face_blocks, owner_rank, owner_tile, live_count, right_side, diagonal):
    blocks = face_blocks.shape[3]
    cx, cy, cz = right_side.shape
    group = sizes["gx"]
    stages = stages_of(sizes)
    slots = sum(len(offsets_of(sizes, axes)) for axes in stages)
    smem, vmem, anywhere = (
        pl.BlockSpec(memory_space=space) for space in (pltpu.SMEM, pltpu.VMEM, pl.ANY)
    )
    box = jax.ShapeDtypeStruct((cx, cy, cz), F32)
    load, p, q, coef = pl.pallas_call(
        functools.partial(kernel, sizes, stages),
        out_shape=(box, box, box, jax.ShapeDtypeStruct((8, cz), F32)),
        in_specs=[smem] * 2 + [anywhere] * 4,
        out_specs=(anywhere, anywhere, anywhere, vmem),
        scratch_shapes=[
            pltpu.SMEM(live_count.shape, jnp.int32),
            pltpu.VMEM((blocks, 2 * cy, cz), F32),
            pltpu.VMEM((cx, cy, cz), F32),
            pltpu.VMEM((cx, cy, cz), F32),
            pltpu.VMEM((cx, cy, cz), F32),
            pltpu.VMEM((cx, cy, cz), F32),
            pltpu.VMEM((blocks * cy, cz), F32),
            pltpu.VMEM((group, cy + 8, cz), F32),
            pltpu.VMEM((group, cy + 8, cz), F32),
            pltpu.VMEM((group, cy + 8, cz), F32),
            pltpu.VMEM((2, 2, cy, cz), F32),
            pltpu.VMEM((2, 2, cx, cz), F32),
            pltpu.VMEM((2, 2, cx, cz), F32),
            pltpu.VMEM((2, cy, cz), F32),
            pltpu.VMEM((2, 2, cy, cz), F32),
            pltpu.VMEM((len(stages), 8, cz), F32),
            pltpu.VMEM((slots, 8, cz), F32),
            pltpu.SemaphoreType.DMA((4,)),
            pltpu.SemaphoreType.DMA((3,)),
            pltpu.SemaphoreType.DMA((group,)),
            pltpu.SemaphoreType.DMA((group,)),
            pltpu.SemaphoreType.DMA((2, 6)),
            pltpu.SemaphoreType.DMA((2, 6)),
            pltpu.SemaphoreType.DMA((slots,)),
            pltpu.SemaphoreType.DMA((slots,)),
        ],
        compiler_params=pltpu.CompilerParams(collective_id=0, has_side_effects=True),
    )(
        owner_rank.reshape(blocks), owner_tile.reshape(blocks), live_count,
        face_blocks.reshape(blocks, 2 * cy, cz), right_side, diagonal,
    )
    return combined(load, p, q, coef)


def solution(mesh):
    sizes = dict(mesh.shape)
    return jax.shard_map(
        functools.partial(per_device, sizes),
        mesh=mesh,
        in_specs=(
            P("gx", "gy", "gz", None, None),
            P("gx", "gy", "gz", None, None),
            P("gx", "gy", "gz", None),
            P("gx", "gy", "gz"),
            P("gx", "gy", "gz"),
            P("gx", "gy", "gz"),
        ),
        out_specs=(P("gx", "gy", "gz"), P("gx", "gy", "gz")),
        check_vma=False,
    )
```
